32 devices in a mesh: groups: 2 (over y), view: 4 (over z), head: 2 (over x), dp: 2 (over core).
Axes of the slice: x: 2, y: 2, z: 4, core: 2. Of those that a mesh axis runs over, the one named last changes fastest.
Arguments:
- ray_tokens: bfloat16 [512, 1024], P(('groups', 'view', 'dp')), parts along dimension 0, may hold values from -6 to 6
- up_weight: bfloat16 [1024, 4096], P('dp', 'head'), may hold values from -0.1875 to 0.1875
- down_weight: bfloat16 [1024, 4096], P('dp', 'head'), may hold values from -0.09375 to 0.09375
- key_weight: bfloat16 [1024, 5120], P('dp', 'head'), may hold values from -0.1875 to 0.1875
- value_weight: bfloat16 [1024, 5120], P('dp', 'head'), may hold values from -0.1875 to 0.1875
- video_queries: bfloat16 [2048, 5120], P(('groups', 'view', 'dp'), 'head'), parts along dimension 0, may hold values from -204 to 204
- video_keys: bfloat16 [2048, 5120], P(('groups', 'view', 'dp'), 'head'), parts along dimension 0, may hold values from -6 to 6
- video_values: bfloat16 [2048, 5120], P(('groups', 'view', 'dp'), 'head'), parts along dimension 0, may hold values from -6 to 6
- cross_queries: bfloat16 [2048, 5120], P(('groups', 'view', 'dp'), 'head'), parts along dimension 0, may hold values from -204 to 204
Outputs:
- attended: bfloat16 [2048, 5120], P(('groups', 'view', 'dp'), 'head'), parts along dimension 0
The draws below stay inside these ranges and needn't reach their ends.
There are 2 independent parts, one for each index of `groups`. The reference program is written for one: setup_inputs(seed, part) draws one part's arguments, and reference() takes and returns one part's arrays. A program takes and returns all parts, laid end to end along the dimension named above; an argument that names none is the same for every part. Nothing has to cross between parts.
All inputs are finite; a program needn't handle non-finite values.
Results may differ from the reference program's by a relative error of at most 0.025.
Values may be sent and summed in bfloat16 or wider, within the bound.
No kernel may reach another device: no remote copies, remote signals or barrier semaphores. Data moves between devices by JAX's collectives and lax.ppermute only.
A program may use at most 64 MiB of HBM per device.

```python
import jax
import jax.numpy as jnp
from jax import lax

HEAD_DIM = 128
DR = 1024
FFR = 4096
D = 5120
TOKENS = 1024
RAYS = 256


def query_rows(key, row_count, spread):
    first = jax.random.fold_in(key, 0)
    base = jax.random.normal(first, (row_count, D), jnp.float32) * spread
    return jnp.clip(base, -6.0 * spread, 6.0 * spread).astype(jnp.bfloat16)


def draw_video_queries(key, part):
    return query_rows(jax.random.fold_in(key, 11), TOKENS, 2.0)


def draw_cross_queries(key, part):
    return query_rows(jax.random.fold_in(key, 23), TOKENS, 2.0)


def level_of(stream_key, extent, cuts, smallest, largest):
    level, own = 1.0, jax.random.fold_in(stream_key, 6)
    for dim, shards_of in cuts:
        steps = jnp.exp(jax.random.uniform(jax.random.fold_in(own, dim), (shards_of,), jnp.float32, smallest / len(cuts), largest / len(cuts)))
        level = level * jnp.repeat(steps, extent[dim] // shards_of).reshape([-1 if axis == dim else 1 for axis in range(len(extent))])
    return level


def gaussian(key, dims, width, bound, cuts=(), held_as=jnp.bfloat16):
    entries = width * jax.random.normal(key, dims, jnp.float32)
    if cuts:
        entries = entries * level_of(key, dims, cuts, -0.22, 0.18)
    return jnp.clip(entries, -bound, bound).astype(held_as)


def setup_inputs(seed: int = 0, part: int = 0) -> dict:
    key_of = jax.random.split(jax.random.key(seed), 10)
    part_keys = jax.random.split(jax.random.fold_in(key_of[9], part), 10)
    ray_tokens = gaussian(part_keys[0], (RAYS, DR), 1.0, 6.0, ((0, 8),))
    up_weight = gaussian(key_of[1], (DR, FFR), DR ** -0.5, 0.1875, ((0, 2), (1, 2)))
    down_weight = gaussian(key_of[2], (DR, FFR), FFR ** -0.5, 0.09375, ((0, 2), (1, 2)))
    key_weight = gaussian(key_of[3], (DR, D), DR ** -0.5, 0.1875, ((0, 2), (1, 2)))
    value_weight = gaussian(key_of[4], (DR, D), DR ** -0.5, 0.1875, ((0, 2), (1, 2)))
    video_queries = draw_video_queries(jax.random.fold_in(jax.random.fold_in(key_of[9], part), 71), part)
    video_keys = gaussian(part_keys[6], (TOKENS, D), 1.0, 6.0, ((0, 8), (1, 2)))
    video_values = gaussian(part_keys[7], (TOKENS, D), 1.0, 6.0, ((0, 8), (1, 2)))
    cross_queries = draw_cross_queries(jax.random.fold_in(jax.random.fold_in(key_of[9], part), 71), part)
    return dict(ray_tokens=ray_tokens, up_weight=up_weight, down_weight=down_weight, key_weight=key_weight, value_weight=value_weight, video_queries=video_queries, video_keys=video_keys, video_values=video_values, cross_queries=cross_queries)


epsilon = 1e-06

def rms_normed(values_in):
    widened = values_in.astype(jnp.float32)
    mean_square = lax.optimization_barrier(jnp.mean(widened * widened, axis=1, keepdims=True))
    return widened * lax.rsqrt(mean_square + epsilon)

def attention(queries, keys, value_matrix):
    row_count = queries.shape[0]
    head_count = queries.shape[1] // HEAD_DIM
    query_head_rows = queries.reshape(row_count, head_count, HEAD_DIM).transpose(1, 0, 2)
    key_head_rows = keys.reshape(keys.shape[0], head_count, HEAD_DIM).transpose(1, 0, 2)
    value_head_rows = value_matrix.reshape(value_matrix.shape[0], head_count, HEAD_DIM).transpose(1, 0, 2)

    def per_head(operands):
        query_head, key_head, value_head = operands
        scores = jnp.dot(query_head, key_head.T, preferred_element_type=jnp.float32) * HEAD_DIM ** (-0.5)
        largest_score = lax.optimization_barrier(jnp.max(scores, axis=1, keepdims=True))
        weights = jnp.exp(scores - largest_score)
        row_sums = lax.optimization_barrier(jnp.sum(weights, axis=1, keepdims=True))
        mixed = jnp.dot(weights.astype(jnp.bfloat16), value_head, preferred_element_type=jnp.float32)
        return mixed / row_sums
    result = lax.map(per_head, (query_head_rows, key_head_rows, value_head_rows))
    return result.transpose(1, 0, 2).reshape(row_count, head_count * HEAD_DIM)

def reference(ray_tokens, up_weight, down_weight, key_weight, value_weight, video_queries, video_keys, video_values, cross_queries):
    normed = rms_normed(ray_tokens).astype(jnp.bfloat16)
    hidden = jax.nn.gelu(jnp.dot(normed, up_weight, preferred_element_type=jnp.float32)).astype(jnp.bfloat16)
    branch = jnp.dot(hidden, down_weight.T, preferred_element_type=jnp.float32)
    rays = (ray_tokens.astype(jnp.float32) + branch).astype(jnp.bfloat16)
    ray_keys = jnp.dot(rays, key_weight, preferred_element_type=jnp.float32).astype(jnp.bfloat16)
    ray_values = jnp.dot(rays, value_weight, preferred_element_type=jnp.float32).astype(jnp.bfloat16)
    own = attention(video_queries, video_keys, video_values)
    cross = attention(cross_queries, ray_keys, ray_values)
    return (own + cross).astype(jnp.bfloat16)
```

```python
import functools

import jax
import jax.numpy as jnp
from jax import lax
from jax.experimental import pallas as pl
from jax.experimental.pallas import tpu as pltpu
from jax.sharding import PartitionSpec as P

HEAD_DIM = 128
SCALE = HEAD_DIM ** (-0.5)


epsilon = 1e-06


def rms_normed(values_in):
    widened = values_in.astype(jnp.float32)
    mean_square = jnp.mean(widened * widened, axis=1, keepdims=True)
    return widened * lax.rsqrt(mean_square + epsilon)


def empty_state(head_count, row_count):
    running_max = jnp.full((head_count, row_count), -1e30, jnp.float32)
    running_sum = jnp.zeros((head_count, row_count), jnp.float32)
    weighted = jnp.zeros((head_count, row_count, HEAD_DIM), jnp.float32)
    return (running_max, running_sum, weighted)


def absorb(state_now, query_head_rows, key_piece, value_piece):
    running_max, running_sum, weighted = state_now
    head_count = query_head_rows.shape[1]
    key_head_rows = key_piece.reshape(key_piece.shape[0], head_count, HEAD_DIM)
    value_head_rows = value_piece.reshape(value_piece.shape[0], head_count, HEAD_DIM)
    scores = jnp.einsum(
        "xrz,frz->rxf", query_head_rows, key_head_rows, preferred_element_type=jnp.float32
    ) * HEAD_DIM ** (-0.5)
    new_max = jnp.maximum(running_max, jnp.max(scores, axis=2))
    exponent = jnp.exp(scores - new_max[:, :, None])
    running_sum = jnp.sum(exponent, axis=2)
    weighted = jnp.einsum(
        "bau,uby->bay",
        exponent.astype(jnp.bfloat16),
        value_head_rows,
        preferred_element_type=jnp.float32,
    )
    return (new_max, running_sum, weighted)


def finish(state_now):
    running_max, running_sum, weighted = state_now
    result = weighted / running_sum[:, :, None]
    head_count, row_count = running_sum.shape
    return result.transpose(1, 0, 2).reshape(row_count, head_count * HEAD_DIM)


def gathered_body(
    ray_tokens,
    up_weight,
    down_weight,
    key_weight,
    value_weight,
    video_queries,
    video_keys,
    video_values,
    cross_queries,
):
    row_count = video_queries.shape[0]
    head_count = video_queries.shape[1] // HEAD_DIM
    up_full, down_full, key_full, value_full = (
        lax.all_gather(up_weight, "dp", axis=0, tiled=True),
        lax.all_gather(down_weight, "dp", axis=0, tiled=True),
        lax.all_gather(key_weight, "dp", axis=0, tiled=True),
        lax.all_gather(value_weight, "dp", axis=0, tiled=True),
    )
    normed = rms_normed(ray_tokens).astype(jnp.bfloat16)
    hidden = jax.nn.gelu(jnp.dot(normed, up_full, preferred_element_type=jnp.float32)).astype(
        jnp.bfloat16
    )
    partial_branch = lax.dot_general(
        hidden, down_full, (((1,), (1,)), ((), ())), preferred_element_type=jnp.float32
    )
    branch = lax.psum(partial_branch, "head")
    rays = (ray_tokens.astype(jnp.float32) + branch).astype(jnp.bfloat16)
    cross_heads = cross_queries.reshape(row_count, head_count, HEAD_DIM)
    piece = lax.all_gather(rays, ("view", "dp"), axis=0, tiled=True)
    piece_keys = jnp.dot(piece, key_full, preferred_element_type=jnp.float32).astype(jnp.bfloat16)
    piece_values = jnp.dot(piece, value_full, preferred_element_type=jnp.float32).astype(
        jnp.bfloat16
    )
    cross_state = absorb(empty_state(head_count, row_count), cross_heads, piece_keys, piece_values)
    cross = finish(cross_state)
    local_head_group = video_queries.reshape(row_count, head_count, HEAD_DIM)
    own_state = absorb(
        empty_state(head_count, row_count),
        local_head_group,
        lax.all_gather(video_keys, ("view", "dp"), axis=0, tiled=True),
        lax.all_gather(video_values, ("view", "dp"), axis=0, tiled=True),
    )
    own = finish(own_state)
    return (own + cross).astype(jnp.bfloat16)


def matmul(left, right):
    return jnp.dot(left, right, preferred_element_type=jnp.float32)


def matmul_t(left, right):
    return lax.dot_general(
        left, right, (((1,), (1,)), ((), ())), preferred_element_type=jnp.float32
    )


def attend(query, keys, values):
    scores = matmul_t(query, keys) * SCALE
    largest = jnp.max(scores, axis=1, keepdims=True)
    weights = jnp.exp(scores - largest)
    total = jnp.sum(weights, axis=1, keepdims=True)
    return matmul(weights.astype(jnp.bfloat16), values) / total


def own_kernel(views, *refs):
    queries = refs[:views]
    pairs = refs[views : 3 * views]
    results = refs[3 * views :]
    keys = jnp.concatenate([pair[0] for pair in pairs], axis=0)
    values = jnp.concatenate([pair[1] for pair in pairs], axis=0)
    for query, result in zip(queries, results):
        result[...] = attend(query[...], keys, values).astype(jnp.bfloat16)


def own_attention(queries, pairs):
    views = len(queries)
    rows, width = queries[0].shape
    heads = width // HEAD_DIM
    key_rows = sum(pair.shape[1] for pair in pairs)
    block = pl.BlockSpec((rows, HEAD_DIM), lambda i: (0, i))
    pair_block = pl.BlockSpec((2, rows, HEAD_DIM), lambda i: (0, 0, i))
    area = views * rows * key_rows * heads
    return pl.pallas_call(
        functools.partial(own_kernel, views),
        grid=(heads,),
        in_specs=[block] * views + [pair_block] * len(pairs),
        out_specs=[block] * views,
        out_shape=[jax.ShapeDtypeStruct((rows, width), jnp.bfloat16)] * views,
        cost_estimate=pl.CostEstimate(
            flops=4 * area * HEAD_DIM,
            transcendentals=area,
            bytes_accessed=2 * width * (2 * views * rows + 2 * key_rows),
        ),
        name="own_attention",
    )(*queries, *pairs)


def cross_kernel(heads, near, far, key_near, key_far, value_near, value_far, query, result):
    ray_near, ray_far = near[...], far[...]
    keys = (matmul(ray_near, key_near[...]) + matmul(ray_far, key_far[...])).astype(jnp.bfloat16)
    values = (matmul(ray_near, value_near[...]) + matmul(ray_far, value_far[...])).astype(
        jnp.bfloat16
    )
    for head in range(heads):
        columns = slice(head * HEAD_DIM, (head + 1) * HEAD_DIM)
        result[:, columns] = attend(query[:, columns], keys[:, columns], values[:, columns])


def cross_attention(near, far, weights, queries):
    rows, width = queries.shape
    ray_rows, depth = near.shape
    heads = 2 if (width // HEAD_DIM) % 2 == 0 else 1
    step = heads * HEAD_DIM
    whole = pl.BlockSpec((ray_rows, depth), lambda i: (0, 0))
    weight_block = pl.BlockSpec((depth, step), lambda i: (0, i))
    block = pl.BlockSpec((rows, step), lambda i: (0, i))
    return pl.pallas_call(
        functools.partial(cross_kernel, heads),
        grid=(width // step,),
        in_specs=[whole, whole] + [weight_block] * 4 + [block],
        out_specs=block,
        out_shape=jax.ShapeDtypeStruct((rows, width), jnp.float32),
        cost_estimate=pl.CostEstimate(
            flops=8 * ray_rows * depth * width + 4 * rows * ray_rows * width,
            transcendentals=rows * ray_rows * width // HEAD_DIM,
            bytes_accessed=8 * depth * width + 6 * rows * width,
        ),
        name="cross_attention",
    )(near, far, *weights, queries)


def join_kernel(views, offsets, span, view, cross, *refs):
    pieces, result = refs[:-1], refs[-1]
    for index, piece in enumerate(pieces):
        chunk, step = divmod(index, views)
        start = pl.multiple_of((view[0] ^ step) * span + offsets[chunk], HEAD_DIM)
        columns = pl.ds(start, piece.shape[1])
        result[:, columns] = (cross[:, columns] + piece[...].astype(jnp.float32)).astype(
            jnp.bfloat16
        )


def join(view, cross, chunks, offsets, span):
    pieces = [piece for chunk in chunks for piece in chunk]
    views = len(chunks[0])
    full = pl.BlockSpec(memory_space=pltpu.VMEM)
    return pl.pallas_call(
        functools.partial(join_kernel, views, offsets, span),
        in_specs=[pl.BlockSpec(memory_space=pltpu.SMEM)] + [full] * (1 + len(pieces)),
        out_specs=full,
        out_shape=jax.ShapeDtypeStruct(cross.shape, jnp.bfloat16),
        cost_estimate=pl.CostEstimate(
            flops=2 * cross.size, transcendentals=0, bytes_accessed=8 * cross.size
        ),
        name="join",
    )(view.reshape(1), cross, *pieces)


def swapped(values, axis):
    return lax.ppermute(values, axis, [(0, 1), (1, 0)])


def exchanged(values, views, step):
    return lax.ppermute(values, "view", [(i, i ^ step) for i in range(views)])


def exchanged_body(
    views,
    ray_tokens,
    up_weight,
    down_weight,
    key_weight,
    value_weight,
    video_queries,
    video_keys,
    video_values,
    cross_queries,
):
    view, side, core = (lax.axis_index(axis) for axis in ("view", "head", "dp"))
    span = video_queries.shape[1] // views
    heads = span // HEAD_DIM
    first = (heads + 1) // 2
    widths = [count * HEAD_DIM for count in (first, heads - first) if count]
    offsets = [sum(widths[:index]) for index in range(len(widths))]
    aligned = side == core

    def pick(values, step, offset, width):
        start = (view ^ step) * span + offset
        return lax.dynamic_slice(values, (0, start), (values.shape[0], width))

    half = ray_tokens.shape[1] // 2
    ray_half = lax.dynamic_slice(ray_tokens, (0, side * half), (ray_tokens.shape[0], half))
    ray_rows = jnp.concatenate(
        [ray_half] + [exchanged(ray_half, views, step) for step in range(1, views)], axis=0
    )
    up_peer, down_peer, key_peer, value_peer = (
        swapped(weight, "dp") for weight in (up_weight, down_weight, key_weight, value_weight)
    )

    chunk_queries, chunk_pairs = [], []
    for offset, width in zip(offsets, widths):
        queries, pairs = [], []
        for step in range(views):
            pair = jnp.stack(
                [pick(video_keys, step, offset, width), pick(video_values, step, offset, width)]
            )
            pairs.append(exchanged(pair, views, step) if step else pair)
        for step in range(views):
            query = pick(video_queries, step, offset, width)
            queries.append(exchanged(query, views, step) if step else query)
        chunk_queries.append(queries)
        chunk_pairs.append(pairs + [swapped(pair, "dp") for pair in pairs])

    other_half = swapped(ray_rows, "head")
    near = jnp.where(aligned, ray_rows, other_half).astype(jnp.float32)
    far = jnp.where(aligned, other_half, ray_rows).astype(jnp.float32)
    square = jnp.sum(near * near, axis=1, keepdims=True) + jnp.sum(far * far, axis=1, keepdims=True)
    factor = lax.rsqrt(square / ray_tokens.shape[1] + epsilon)
    hidden = jax.nn.gelu(
        matmul((near * factor).astype(jnp.bfloat16), up_weight)
        + matmul((far * factor).astype(jnp.bfloat16), up_peer)
    ).astype(jnp.bfloat16)
    branch_near = matmul_t(hidden, down_weight)
    branch_far = matmul_t(hidden, down_peer)
    branch = jnp.where(aligned, branch_near, branch_far) + swapped(
        jnp.where(aligned, branch_far, branch_near), "head"
    )
    rays_here = (ray_rows.astype(jnp.float32) + branch).astype(jnp.bfloat16)
    rays_there = swapped(rays_here, "head")
    rays_near = jnp.where(aligned, rays_here, rays_there)
    rays_far = jnp.where(aligned, rays_there, rays_here)
    all_near = jnp.concatenate([rays_near, swapped(rays_far, "dp")], axis=0)
    all_far = jnp.concatenate([rays_far, swapped(rays_near, "dp")], axis=0)
    cross = cross_attention(
        all_near, all_far, (key_weight, key_peer, value_weight, value_peer), cross_queries
    )

    returned = []
    for queries, pairs in zip(chunk_queries, chunk_pairs):
        results = own_attention(queries, pairs)
        returned.append(
            [exchanged(part, views, step) if step else part for step, part in enumerate(results)]
        )
    return join(view, cross, returned, offsets, span)


def solution(mesh):
    row_axes = ("groups", "view", "dp")
    in_specs = (P(row_axes, None),) + (P("dp", "head"),) * 4 + (P(row_axes, "head"),) * 4
    out_specs = P(row_axes, "head")

    def whole(*arrays):
        views = mesh.shape["view"]
        heads = arrays[5].shape[1] // HEAD_DIM // mesh.shape["head"]
        exchange = (
            mesh.shape["dp"] == 2
            and mesh.shape["head"] == 2
            and views > 1
            and views & (views - 1) == 0
            and heads % views == 0
        )
        body = functools.partial(exchanged_body, views) if exchange else gathered_body
        return jax.shard_map(
            body, mesh=mesh, in_specs=in_specs, out_specs=out_specs, check_vma=False
        )(*arrays)

    return whole
```

```python
import functools
import math

import jax
import jax.numpy as jnp
from jax import lax
from jax.experimental import pallas as pl
from jax.experimental.pallas import tpu as pltpu
from jax.sharding import PartitionSpec as P

HEAD_DIM = 128
EXPONENT = HEAD_DIM ** (-0.5) * math.log2(math.e)


epsilon = 1e-06


def rms_normed(values_in):
    widened = values_in.astype(jnp.float32)
    mean_square = jnp.mean(widened * widened, axis=1, keepdims=True)
    return widened * lax.rsqrt(mean_square + epsilon)


def empty_state(head_count, row_count):
    running_max = jnp.full((head_count, row_count), -1e30, jnp.float32)
    running_sum = jnp.zeros((head_count, row_count), jnp.float32)
    weighted = jnp.zeros((head_count, row_count, HEAD_DIM), jnp.float32)
    return (running_max, running_sum, weighted)


def absorb(state_now, query_head_rows, key_piece, value_piece):
    running_max, running_sum, weighted = state_now
    head_count = query_head_rows.shape[1]
    key_head_rows = key_piece.reshape(key_piece.shape[0], head_count, HEAD_DIM)
    value_head_rows = value_piece.reshape(value_piece.shape[0], head_count, HEAD_DIM)
    scores = jnp.einsum(
        "xrz,frz->rxf", query_head_rows, key_head_rows, preferred_element_type=jnp.float32
    ) * HEAD_DIM ** (-0.5)
    new_max = jnp.maximum(running_max, jnp.max(scores, axis=2))
    exponent = jnp.exp(scores - new_max[:, :, None])
    running_sum = jnp.sum(exponent, axis=2)
    weighted = jnp.einsum(
        "bau,uby->bay",
        exponent.astype(jnp.bfloat16),
        value_head_rows,
        preferred_element_type=jnp.float32,
    )
    return (new_max, running_sum, weighted)


def finish(state_now):
    _, running_sum, weighted = state_now
    result = weighted / running_sum[:, :, None]
    head_count, row_count = running_sum.shape
    return result.transpose(1, 0, 2).reshape(row_count, head_count * HEAD_DIM)


def gathered_body(
    ray_tokens,
    up_weight,
    down_weight,
    key_weight,
    value_weight,
    video_queries,
    video_keys,
    video_values,
    cross_queries,
):
    row_count = video_queries.shape[0]
    head_count = video_queries.shape[1] // HEAD_DIM
    up_full, down_full, key_full, value_full = (
        lax.all_gather(up_weight, "dp", axis=0, tiled=True),
        lax.all_gather(down_weight, "dp", axis=0, tiled=True),
        lax.all_gather(key_weight, "dp", axis=0, tiled=True),
        lax.all_gather(value_weight, "dp", axis=0, tiled=True),
    )
    normed = rms_normed(ray_tokens).astype(jnp.bfloat16)
    hidden = jax.nn.gelu(jnp.dot(normed, up_full, preferred_element_type=jnp.float32)).astype(
        jnp.bfloat16
    )
    partial_branch = lax.dot_general(
        hidden, down_full, (((1,), (1,)), ((), ())), preferred_element_type=jnp.float32
    )
    branch = lax.psum(partial_branch, "head")
    rays = (ray_tokens.astype(jnp.float32) + branch).astype(jnp.bfloat16)
    cross_heads = cross_queries.reshape(row_count, head_count, HEAD_DIM)
    piece = lax.all_gather(rays, ("view", "dp"), axis=0, tiled=True)
    piece_keys = jnp.dot(piece, key_full, preferred_element_type=jnp.float32).astype(jnp.bfloat16)
    piece_values = jnp.dot(piece, value_full, preferred_element_type=jnp.float32).astype(
        jnp.bfloat16
    )
    cross_state = absorb(empty_state(head_count, row_count), cross_heads, piece_keys, piece_values)
    cross = finish(cross_state)
    local_head_group = video_queries.reshape(row_count, head_count, HEAD_DIM)
    own_state = absorb(
        empty_state(head_count, row_count),
        local_head_group,
        lax.all_gather(video_keys, ("view", "dp"), axis=0, tiled=True),
        lax.all_gather(video_values, ("view", "dp"), axis=0, tiled=True),
    )
    own = finish(own_state)
    return (own + cross).astype(jnp.bfloat16)


VMEM = pl.BlockSpec(memory_space=pltpu.VMEM)
HBM = pl.BlockSpec(memory_space=pltpu.HBM)
SMEM = pl.BlockSpec(memory_space=pltpu.SMEM)
MIB = 2**20


def local_call(
    kernel, megabytes, flops, transcendentals, out_shape, scalars, *arrays, streamed=(), scratch=()
):
    moved = sum(array.size * array.dtype.itemsize for array in arrays + tuple(streamed))
    call = pl.pallas_call(
        kernel,
        in_specs=[SMEM] * len(scalars) + [VMEM] * len(arrays) + [HBM] * len(streamed),
        scratch_shapes=list(scratch),
        out_specs=jax.tree.map(lambda _: VMEM, out_shape),
        out_shape=out_shape,
        cost_estimate=pl.CostEstimate(
            flops=flops, transcendentals=transcendentals, bytes_accessed=moved
        ),
        compiler_params=pltpu.CompilerParams(vmem_limit_bytes=megabytes * MIB),
    )
    scalars = (scalar.astype(jnp.int32).reshape(1) for scalar in scalars)
    streamed = (pltpu.with_memory_space_constraint(array, pltpu.HBM) for array in streamed)
    return call(*scalars, *arrays, *streamed)


def matmul(left, right):
    return jnp.dot(left, right, preferred_element_type=jnp.float32)


def matmul_t(left, right):
    return lax.dot_general(
        left, right, (((1,), (1,)), ((), ())), preferred_element_type=jnp.float32
    )


def attend(query, keys, values):
    scores = matmul_t(query, keys)
    largest = jnp.max(scores, axis=1, keepdims=True)
    weights = jnp.exp2((scores - largest) * EXPONENT)
    total = jnp.sum(weights, axis=1, keepdims=True)
    return matmul(weights.astype(jnp.bfloat16), values) / total


def head_columns(head):
    return pl.ds(pl.multiple_of(head * HEAD_DIM, HEAD_DIM), HEAD_DIM)


def pack_kernel(views, offset, view, *refs):
    sources, results, arrived = refs[:3], refs[3:-1], refs[-1]
    span = sources[0].shape[1] // views
    copies = []
    for step, result in enumerate(results):
        start = pl.multiple_of((view[0] ^ step) * span + offset, HEAD_DIM)
        for slot, source in enumerate(sources):
            copies.append(
                pltpu.make_async_copy(
                    source.at[:, pl.ds(start, result.shape[2])],
                    result.at[slot],
                    arrived.at[step, slot],
                )
            )
    for copy in copies:
        copy.start()
    for copy in copies:
        copy.wait()


def pack(view, views, offset, width, keys, values, queries):
    rows = keys.shape[0]
    return local_call(
        functools.partial(pack_kernel, views, offset),
        8,
        keys.size,
        0,
        [jax.ShapeDtypeStruct((3, rows, width), jnp.bfloat16)] * views,
        (view,),
        streamed=(keys, values, queries),
        scratch=(pltpu.SemaphoreType.DMA((views, 3)),),
    )


def ray_kernel(aligned, here_ref, there_ref, *refs):
    sources, (keep, send), held, arrived = refs[:4], refs[4:6], refs[6:10], refs[10]
    copies = [
        pltpu.make_async_copy(source, target, arrived.at[index])
        for index, (source, target) in enumerate(zip(sources, held))
    ]
    for copy in copies:
        copy.start()
    same = aligned[0] == 1
    here, there = here_ref[...].astype(jnp.float32), there_ref[...].astype(jnp.float32)
    square = jnp.sum(here * here + there * there, axis=1, keepdims=True)
    factor = lax.rsqrt(square / (2 * here.shape[1]) + epsilon)
    here = (here * factor).astype(jnp.bfloat16)
    there = (there * factor).astype(jnp.bfloat16)
    near, far = jnp.where(same, here, there), jnp.where(same, there, here)
    copies[0].wait()
    copies[1].wait()
    hidden = jax.nn.gelu(matmul(near, held[0][...]) + matmul(far, held[1][...]))
    hidden = hidden.astype(jnp.bfloat16)
    copies[2].wait()
    branch_near = matmul_t(hidden, held[2][...])
    copies[3].wait()
    branch_far = matmul_t(hidden, held[3][...])
    keep[...] = jnp.where(same, branch_near, branch_far) + here_ref[...].astype(jnp.float32)
    send[...] = jnp.where(same, branch_far, branch_near)


def ray_layer(aligned, here, there, weights):
    return local_call(
        ray_kernel,
        20,
        8 * here.size * weights[0].shape[1],
        0,
        [jax.ShapeDtypeStruct(here.shape, jnp.float32)] * 2,
        (aligned,),
        here,
        there,
        streamed=weights,
        scratch=[pltpu.VMEM(weight.shape, weight.dtype) for weight in weights]
        + [pltpu.SemaphoreType.DMA((4,))],
    )


def own_kernel(views, *refs):
    pieces, others, results = refs[:views], refs[views : 2 * views], refs[2 * views :]

    @pl.loop(0, results[0].shape[1] // HEAD_DIM)
    def _(head):
        columns = head_columns(head)
        keys = jnp.concatenate([piece[0, :, columns] for piece in pieces + others], axis=0)
        values = jnp.concatenate([piece[1, :, columns] for piece in pieces + others], axis=0)
        for piece, result in zip(pieces, results):
            result[:, columns] = attend(piece[2, :, columns], keys, values).astype(jnp.bfloat16)


def own_attention(pieces, others):
    views = len(pieces)
    _, rows, width = pieces[0].shape
    area = 2 * views * views * rows * rows * (width // HEAD_DIM)
    out_shape = [jax.ShapeDtypeStruct((rows, width), jnp.bfloat16)] * views
    kernel = functools.partial(own_kernel, views)
    return local_call(kernel, 12, 4 * area * HEAD_DIM, area, out_shape, (), *pieces, *others)


def cross_kernel(
    heads,
    aligned,
    here,
    there,
    peer_here,
    peer_there,
    key_near,
    key_far,
    value_near,
    value_far,
    query,
    result,
):
    same = aligned[0] == 1
    first = jnp.concatenate([here[...], peer_here[...]], axis=0)
    second = jnp.concatenate([there[...], peer_there[...]], axis=0)
    near, far = jnp.where(same, first, second), jnp.where(same, second, first)
    step = heads * HEAD_DIM

    @pl.loop(0, query.shape[1] // step)
    def _(group):
        block = pl.ds(pl.multiple_of(group * step, step), step)
        keys = (matmul(near, key_near[:, block]) + matmul(far, key_far[:, block])).astype(
            jnp.bfloat16
        )
        values = (matmul(near, value_near[:, block]) + matmul(far, value_far[:, block])).astype(
            jnp.bfloat16
        )
        for head in range(heads):
            inner = slice(head * HEAD_DIM, (head + 1) * HEAD_DIM)
            outer = head_columns(group * heads + head)
            result[:, outer] = attend(query[:, outer], keys[:, inner], values[:, inner])


def cross_attention(aligned, rays, weights, queries):
    rows, width = queries.shape
    ray_rows, depth = 2 * rays[0].shape[0], rays[0].shape[1]
    count = width // HEAD_DIM
    heads = max(group for group in range(1, 11) if count % group == 0)
    return local_call(
        functools.partial(cross_kernel, heads),
        20,
        8 * ray_rows * depth * width + 4 * rows * ray_rows * width,
        rows * ray_rows * count,
        jax.ShapeDtypeStruct((rows, width), jnp.float32),
        (aligned,),
        *rays,
        *weights,
        queries,
    )


def join_kernel(views, offsets, view, cross, *refs):
    pieces, result = refs[:-1], refs[-1]
    span = cross.shape[1] // views
    for index, piece in enumerate(pieces):
        chunk, step = divmod(index, views)
        start = pl.multiple_of((view[0] ^ step) * span + offsets[chunk], HEAD_DIM)
        columns = pl.ds(start, piece.shape[1])
        result[:, columns] = (cross[:, columns] + piece[...].astype(jnp.float32)).astype(
            jnp.bfloat16
        )


def join(view, cross, chunks, offsets):
    pieces = [piece for chunk in chunks for piece in chunk]
    kernel = functools.partial(join_kernel, len(chunks[0]), offsets)
    out_shape = jax.ShapeDtypeStruct(cross.shape, jnp.bfloat16)
    return local_call(kernel, 6, 2 * cross.size, 0, out_shape, (view,), cross, *pieces)


def swapped(values, axis):
    return lax.ppermute(values, axis, [(0, 1), (1, 0)])


def exchanged(values, views, step):
    return lax.ppermute(values, "view", [(i, i ^ step) for i in range(views)])


def exchanged_body(views, *arrays):
    return exchange_heads(views, *arrays)


def exchange_heads(
    views,
    ray_tokens,
    up_weight,
    down_weight,
    key_weight,
    value_weight,
    video_queries,
    video_keys,
    video_values,
    cross_queries,
):
    view, side, core = (lax.axis_index(axis) for axis in ("view", "head", "dp"))
    span = video_queries.shape[1] // views
    widths, offsets = chunk_columns(span)
    aligned = side == core

    half = ray_tokens.shape[1] // 2
    ray_half = lax.dynamic_slice(ray_tokens, (0, side * half), (ray_tokens.shape[0], half))
    ray_rows = jnp.concatenate(
        [ray_half]
        + [exchanged(ray_half, views, step) for step in range(1, views)],
        axis=0,
    )
    up_peer = swapped(up_weight, "dp")
    down_peer = swapped(down_weight, "dp")
    key_peer = swapped(key_weight, "dp")
    value_peer = swapped(value_weight, "dp")

    packed = [
        pack(view, views, *columns, video_keys, video_values, video_queries)
        for columns in zip(offsets, widths)
    ]
    chunks = [
        [exchanged(piece, views, step) if step else piece for step, piece in enumerate(pieces)]
        for pieces in packed
    ]

    other_half = swapped(ray_rows, "head")
    keep, send = ray_layer(
        aligned, ray_rows, other_half, (up_weight, up_peer, down_weight, down_peer)
    )
    here = (keep + swapped(send, "head")).astype(jnp.bfloat16)
    there = swapped(here, "head")
    rays = (here, there, swapped(here, "dp"), swapped(there, "dp"))
    cross = cross_attention(
        aligned, rays, (key_weight, key_peer, value_weight, value_peer), cross_queries
    )

    returned = []
    for pieces in chunks:
        others = [swapped(piece, "dp") for piece in pieces]
        results = own_attention(pieces, others)
        returned.append(
            [exchanged(part, views, step) if step else part for step, part in enumerate(results)]
        )
    return join(view, cross, returned, offsets)


def chunk_columns(span):
    heads = span // HEAD_DIM
    first = (heads + 1) // 2
    widths = [count * HEAD_DIM for count in (first, heads - first) if count]
    return widths, [sum(widths[:index]) for index in range(len(widths))]


def solution(mesh):
    row_axes = ("groups", "view", "dp")
    in_specs = (P(row_axes, None),) + (P("dp", "head"),) * 4 + (P(row_axes, "head"),) * 4
    out_specs = P(row_axes, "head")

    views = mesh.shape["view"]

    def mapped(body):
        return jax.shard_map(
            body, mesh=mesh, in_specs=in_specs, out_specs=out_specs, check_vma=False
        )

    def whole(*arrays):
        span = arrays[5].shape[1] // mesh.shape["head"] // views
        exchange = (
            mesh.shape["dp"] == 2
            and mesh.shape["head"] == 2
            and views > 1
            and views & (views - 1) == 0
            and span % HEAD_DIM == 0
        )
        if not exchange:
            return mapped(gathered_body)(*arrays)
        step = mapped(functools.partial(exchanged_body, views))
        return step(*arrays)

    return whole
```

```python
import functools
import math

import jax
import jax.numpy as jnp
from jax import lax
from jax.experimental import pallas as pl
from jax.experimental.pallas import tpu as pltpu
from jax.sharding import PartitionSpec as P

HEAD_DIM = 128
EXPONENT = HEAD_DIM ** (-0.5) * math.log2(math.e)


epsilon = 1e-06


def rms_normed(values_in):
    widened = values_in.astype(jnp.float32)
    mean_square = jnp.mean(widened * widened, axis=1, keepdims=True)
    return widened * lax.rsqrt(mean_square + epsilon)


def empty_state(head_count, row_count):
    running_max = jnp.full((head_count, row_count), -1e30, jnp.float32)
    running_sum = jnp.zeros((head_count, row_count), jnp.float32)
    weighted = jnp.zeros((head_count, row_count, HEAD_DIM), jnp.float32)
    return (running_max, running_sum, weighted)


def absorb(state_now, query_head_rows, key_piece, value_piece):
    running_max, running_sum, weighted = state_now
    head_count = query_head_rows.shape[1]
    key_head_rows = key_piece.reshape(key_piece.shape[0], head_count, HEAD_DIM)
    value_head_rows = value_piece.reshape(value_piece.shape[0], head_count, HEAD_DIM)
    scores = jnp.einsum(
        "xrz,frz->rxf", query_head_rows, key_head_rows, preferred_element_type=jnp.float32
    ) * HEAD_DIM ** (-0.5)
    new_max = jnp.maximum(running_max, jnp.max(scores, axis=2))
    exponent = jnp.exp(scores - new_max[:, :, None])
    running_sum = jnp.sum(exponent, axis=2)
    weighted = jnp.einsum(
        "bau,uby->bay",
        exponent.astype(jnp.bfloat16),
        value_head_rows,
        preferred_element_type=jnp.float32,
    )
    return (new_max, running_sum, weighted)


def finish(state_now):
    _, running_sum, weighted = state_now
    result = weighted / running_sum[:, :, None]
    head_count, row_count = running_sum.shape
    return result.transpose(1, 0, 2).reshape(row_count, head_count * HEAD_DIM)


def gathered_body(
    ray_tokens,
    up_weight,
    down_weight,
    key_weight,
    value_weight,
    video_queries,
    video_keys,
    video_values,
    cross_queries,
):
    row_count = video_queries.shape[0]
    head_count = video_queries.shape[1] // HEAD_DIM
    up_full, down_full, key_full, value_full = (
        lax.all_gather(up_weight, "dp", axis=0, tiled=True),
        lax.all_gather(down_weight, "dp", axis=0, tiled=True),
        lax.all_gather(key_weight, "dp", axis=0, tiled=True),
        lax.all_gather(value_weight, "dp", axis=0, tiled=True),
    )
    normed = rms_normed(ray_tokens).astype(jnp.bfloat16)
    hidden = jax.nn.gelu(jnp.dot(normed, up_full, preferred_element_type=jnp.float32)).astype(
        jnp.bfloat16
    )
    partial_branch = lax.dot_general(
        hidden, down_full, (((1,), (1,)), ((), ())), preferred_element_type=jnp.float32
    )
    branch = lax.psum(partial_branch, "head")
    rays = (ray_tokens.astype(jnp.float32) + branch).astype(jnp.bfloat16)
    cross_heads = cross_queries.reshape(row_count, head_count, HEAD_DIM)
    piece = lax.all_gather(rays, ("view", "dp"), axis=0, tiled=True)
    piece_keys = jnp.dot(piece, key_full, preferred_element_type=jnp.float32).astype(jnp.bfloat16)
    piece_values = jnp.dot(piece, value_full, preferred_element_type=jnp.float32).astype(
        jnp.bfloat16
    )
    cross_state = absorb(empty_state(head_count, row_count), cross_heads, piece_keys, piece_values)
    cross = finish(cross_state)
    local_head_group = video_queries.reshape(row_count, head_count, HEAD_DIM)
    own_state = absorb(
        empty_state(head_count, row_count),
        local_head_group,
        lax.all_gather(video_keys, ("view", "dp"), axis=0, tiled=True),
        lax.all_gather(video_values, ("view", "dp"), axis=0, tiled=True),
    )
    own = finish(own_state)
    return (own + cross).astype(jnp.bfloat16)


VMEM = pl.BlockSpec(memory_space=pltpu.VMEM)
HBM = pl.BlockSpec(memory_space=pltpu.HBM)
SMEM = pl.BlockSpec(memory_space=pltpu.SMEM)
MIB = 2**20


def local_call(
    kernel, megabytes, flops, transcendentals, out_shape, scalars, *arrays, streamed=(), scratch=()
):
    moved = sum(array.size * array.dtype.itemsize for array in arrays + tuple(streamed))
    call = pl.pallas_call(
        kernel,
        in_specs=[SMEM] * len(scalars) + [VMEM] * len(arrays) + [HBM] * len(streamed),
        scratch_shapes=list(scratch),
        out_specs=jax.tree.map(lambda _: VMEM, out_shape),
        out_shape=out_shape,
        cost_estimate=pl.CostEstimate(
            flops=flops, transcendentals=transcendentals, bytes_accessed=moved
        ),
        compiler_params=pltpu.CompilerParams(vmem_limit_bytes=megabytes * MIB),
    )
    scalars = (scalar.astype(jnp.int32).reshape(1) for scalar in scalars)
    streamed = (pltpu.with_memory_space_constraint(array, pltpu.HBM) for array in streamed)
    return call(*scalars, *arrays, *streamed)


def matmul(left, right):
    return jnp.dot(left, right, preferred_element_type=jnp.float32)


def matmul_t(left, right):
    return lax.dot_general(
        left, right, (((1,), (1,)), ((), ())), preferred_element_type=jnp.float32
    )


def attend(query, keys, values):
    scores = matmul_t(query, keys)
    largest = jnp.max(scores, axis=1, keepdims=True)
    weights = jnp.exp2((scores - largest) * EXPONENT)
    total = jnp.sum(weights, axis=1, keepdims=True)
    return matmul(weights.astype(jnp.bfloat16), values) / total


def head_columns(head):
    return pl.ds(pl.multiple_of(head * HEAD_DIM, HEAD_DIM), HEAD_DIM)


def pack_kernel(views, offset, view, side, *refs):
    count = (len(refs) - 1 - views + 3) // 2
    sources, results, arrived = refs[:count], refs[count:-1], refs[-1]
    span = sources[0].shape[1] // views
    copies = []
    for step, result in enumerate(results[:views]):
        start = pl.multiple_of((view[0] ^ step) * span + offset, HEAD_DIM)
        for slot, source in enumerate(sources[:3]):
            copies.append(
                pltpu.make_async_copy(
                    source.at[:, pl.ds(start, result.shape[2])],
                    result.at[slot],
                    arrived.at[step, slot],
                )
            )
    for source, result in zip(sources[3:], results[views:]):
        half = result.shape[1]
        start = pl.multiple_of(side[0] * half, HEAD_DIM)
        copies.append(
            pltpu.make_async_copy(source.at[:, pl.ds(start, half)], result, arrived.at[views, 0])
        )
    for copy in copies:
        copy.start()
    for copy in copies:
        copy.wait()


def pack(view, side, views, offset, width, keys, values, queries, *rays):
    rows = keys.shape[0]
    out_shape = [jax.ShapeDtypeStruct((3, rows, width), jnp.bfloat16)] * views
    out_shape += [jax.ShapeDtypeStruct((r.shape[0], r.shape[1] // 2), r.dtype) for r in rays]
    return local_call(
        functools.partial(pack_kernel, views, offset),
        8,
        keys.size,
        0,
        out_shape,
        (view, side),
        streamed=(keys, values, queries, *rays),
        scratch=(pltpu.SemaphoreType.DMA((views + 1, 3)),),
    )


def ray_kernel(aligned, here_ref, there_ref, *refs):
    sources, (keep, send), held, arrived = refs[:4], refs[4:6], refs[6:10], refs[10]
    copies = [
        pltpu.make_async_copy(source, target, arrived.at[index])
        for index, (source, target) in enumerate(zip(sources, held))
    ]
    for copy in copies:
        copy.start()
    same = aligned[0] == 1
    here, there = here_ref[...].astype(jnp.float32), there_ref[...].astype(jnp.float32)
    square = jnp.sum(here * here + there * there, axis=1, keepdims=True)
    factor = lax.rsqrt(square / (2 * here.shape[1]) + epsilon)
    here = (here * factor).astype(jnp.bfloat16)
    there = (there * factor).astype(jnp.bfloat16)
    near, far = jnp.where(same, here, there), jnp.where(same, there, here)
    copies[0].wait()
    copies[1].wait()
    hidden = jax.nn.gelu(matmul(near, held[0][...]) + matmul(far, held[1][...]))
    hidden = hidden.astype(jnp.bfloat16)
    copies[2].wait()
    branch_near = matmul_t(hidden, held[2][...])
    copies[3].wait()
    branch_far = matmul_t(hidden, held[3][...])
    keep[...] = jnp.where(same, branch_near, branch_far) + here_ref[...].astype(jnp.float32)
    send[...] = jnp.where(same, branch_far, branch_near)


def ray_layer(aligned, here, there, weights):
    return local_call(
        ray_kernel,
        20,
        8 * here.size * weights[0].shape[1],
        0,
        [jax.ShapeDtypeStruct(here.shape, jnp.float32)] * 2,
        (aligned,),
        here,
        there,
        streamed=weights,
        scratch=[pltpu.VMEM(weight.shape, weight.dtype) for weight in weights]
        + [pltpu.SemaphoreType.DMA((4,))],
    )


def own_kernel(views, *refs):
    pieces, others, results = refs[:views], refs[views : 2 * views], refs[2 * views :]

    @pl.loop(0, results[0].shape[1] // HEAD_DIM)
    def _(head):
        columns = head_columns(head)
        keys = jnp.concatenate([piece[0, :, columns] for piece in pieces + others], axis=0)
        values = jnp.concatenate([piece[1, :, columns] for piece in pieces + others], axis=0)
        for piece, result in zip(pieces, results):
            result[:, columns] = attend(piece[2, :, columns], keys, values).astype(jnp.bfloat16)


def own_attention(pieces, others):
    views = len(pieces)
    _, rows, width = pieces[0].shape
    area = 2 * views * views * rows * rows * (width // HEAD_DIM)
    out_shape = [jax.ShapeDtypeStruct((rows, width), jnp.bfloat16)] * views
    kernel = functools.partial(own_kernel, views)
    return local_call(kernel, 12, 4 * area * HEAD_DIM, area, out_shape, (), *pieces, *others)


def cross_kernel(
    heads,
    aligned,
    here,
    there,
    peer_here,
    peer_there,
    key_near,
    key_far,
    value_near,
    value_far,
    query,
    result,
):
    same = aligned[0] == 1
    first = jnp.concatenate([here[...], peer_here[...]], axis=0)
    second = jnp.concatenate([there[...], peer_there[...]], axis=0)
    near, far = jnp.where(same, first, second), jnp.where(same, second, first)
    step = heads * HEAD_DIM

    @pl.loop(0, query.shape[1] // step)
    def _(group):
        block = pl.ds(pl.multiple_of(group * step, step), step)
        keys = (matmul(near, key_near[:, block]) + matmul(far, key_far[:, block])).astype(
            jnp.bfloat16
        )
        values = (matmul(near, value_near[:, block]) + matmul(far, value_far[:, block])).astype(
            jnp.bfloat16
        )
        for head in range(heads):
            inner = slice(head * HEAD_DIM, (head + 1) * HEAD_DIM)
            outer = head_columns(group * heads + head)
            result[:, outer] = attend(query[:, outer], keys[:, inner], values[:, inner])


def cross_attention(aligned, rays, weights, queries):
    rows, width = queries.shape
    ray_rows, depth = 2 * rays[0].shape[0], rays[0].shape[1]
    count = width // HEAD_DIM
    heads = max(group for group in range(1, 11) if count % group == 0)
    return local_call(
        functools.partial(cross_kernel, heads),
        20,
        8 * ray_rows * depth * width + 4 * rows * ray_rows * width,
        rows * ray_rows * count,
        jax.ShapeDtypeStruct((rows, width), jnp.float32),
        (aligned,),
        *rays,
        *weights,
        queries,
    )


def join_kernel(views, offsets, view, cross, *refs):
    pieces, result = refs[:-1], refs[-1]
    span = cross.shape[1] // views
    for index, piece in enumerate(pieces):
        chunk, step = divmod(index, views)
        start = pl.multiple_of((view[0] ^ step) * span + offsets[chunk], HEAD_DIM)
        columns = pl.ds(start, piece.shape[1])
        result[:, columns] = (cross[:, columns] + piece[...].astype(jnp.float32)).astype(
            jnp.bfloat16
        )


def join(view, cross, chunks, offsets):
    pieces = [piece for chunk in chunks for piece in chunk]
    kernel = functools.partial(join_kernel, len(chunks[0]), offsets)
    out_shape = jax.ShapeDtypeStruct(cross.shape, jnp.bfloat16)
    return local_call(kernel, 6, 2 * cross.size, 0, out_shape, (view,), cross, *pieces)


def swapped(values, axis):
    return lax.ppermute(values, axis, [(0, 1), (1, 0)])


def exchanged(values, views, step):
    return lax.ppermute(values, "view", [(i, i ^ step) for i in range(views)])


def exchanged_body(views, *arrays):
    return exchange_heads(views, *arrays)


def exchange_heads(
    views,
    ray_tokens,
    up_weight,
    down_weight,
    key_weight,
    value_weight,
    video_queries,
    video_keys,
    video_values,
    cross_queries,
):
    view, side, core = (lax.axis_index(axis) for axis in ("view", "head", "dp"))
    span = video_queries.shape[1] // views
    widths, offsets = chunk_columns(span)
    aligned = side == core

    packed = []
    for index, columns in enumerate(zip(offsets, widths)):
        extra = () if index else (ray_tokens,)
        packed.append(
            pack(view, side, views, *columns, video_keys, video_values, video_queries, *extra)
        )
    ray_half = packed[0][views]
    ray_rows = jnp.concatenate(
        [ray_half]
        + [exchanged(ray_half, views, step) for step in range(1, views)],
        axis=0,
    )
    up_peer = swapped(up_weight, "dp")
    down_peer = swapped(down_weight, "dp")
    key_peer = swapped(key_weight, "dp")
    value_peer = swapped(value_weight, "dp")

    chunks = [
        [
            exchanged(piece, views, step) if step else piece
            for step, piece in enumerate(pieces[:views])
        ]
        for pieces in packed
    ]

    other_half = swapped(ray_rows, "head")
    keep, send = ray_layer(
        aligned, ray_rows, other_half, (up_weight, up_peer, down_weight, down_peer)
    )
    here = (keep + swapped(send, "head")).astype(jnp.bfloat16)
    there = swapped(here, "head")
    rays = (here, there, swapped(here, "dp"), swapped(there, "dp"))
    cross = cross_attention(
        aligned, rays, (key_weight, key_peer, value_weight, value_peer), cross_queries
    )

    returned = []
    for pieces in chunks:
        others = [swapped(piece, "dp") for piece in pieces]
        results = own_attention(pieces, others)
        returned.append(
            [exchanged(part, views, step) if step else part for step, part in enumerate(results)]
        )
    return join(view, cross, returned, offsets)


def chunk_columns(span):
    heads = span // HEAD_DIM
    first = (heads + 1) // 2
    widths = [count * HEAD_DIM for count in (first, heads - first) if count]
    return widths, [sum(widths[:index]) for index in range(len(widths))]


def solution(mesh):
    row_axes = ("groups", "view", "dp")
    in_specs = (P(row_axes, None),) + (P("dp", "head"),) * 4 + (P(row_axes, "head"),) * 4
    out_specs = P(row_axes, "head")

    views = mesh.shape["view"]

    def mapped(body):
        return jax.shard_map(
            body, mesh=mesh, in_specs=in_specs, out_specs=out_specs, check_vma=False
        )

    def whole(*arrays):
        span = arrays[5].shape[1] // mesh.shape["head"] // views
        exchange = (
            mesh.shape["dp"] == 2
            and mesh.shape["head"] == 2
            and views > 1
            and views & (views - 1) == 0
            and span % HEAD_DIM == 0
        )
        if not exchange:
            return mapped(gathered_body)(*arrays)
        step = mapped(functools.partial(exchanged_body, views))
        return step(*arrays)

    return whole
```

```python
import functools
import math

import jax
import jax.numpy as jnp
from jax import lax
from jax.experimental import pallas as pl
from jax.experimental.pallas import tpu as pltpu
from jax.sharding import PartitionSpec as P

HEAD_DIM = 128
EXPONENT = HEAD_DIM ** (-0.5) * math.log2(math.e)


epsilon = 1e-06


def rms_normed(values_in):
    widened = values_in.astype(jnp.float32)
    mean_square = jnp.mean(widened * widened, axis=1, keepdims=True)
    return widened * lax.rsqrt(mean_square + epsilon)


def empty_state(head_count, row_count):
    running_max = jnp.full((head_count, row_count), -1e30, jnp.float32)
    running_sum = jnp.zeros((head_count, row_count), jnp.float32)
    weighted = jnp.zeros((head_count, row_count, HEAD_DIM), jnp.float32)
    return (running_max, running_sum, weighted)


def absorb(state_now, query_head_rows, key_piece, value_piece):
    running_max, running_sum, weighted = state_now
    head_count = query_head_rows.shape[1]
    key_head_rows = key_piece.reshape(key_piece.shape[0], head_count, HEAD_DIM)
    value_head_rows = value_piece.reshape(value_piece.shape[0], head_count, HEAD_DIM)
    scores = jnp.einsum(
        "xrz,frz->rxf", query_head_rows, key_head_rows, preferred_element_type=jnp.float32
    ) * HEAD_DIM ** (-0.5)
    new_max = jnp.maximum(running_max, jnp.max(scores, axis=2))
    exponent = jnp.exp(scores - new_max[:, :, None])
    running_sum = jnp.sum(exponent, axis=2)
    weighted = jnp.einsum(
        "bau,uby->bay",
        exponent.astype(jnp.bfloat16),
        value_head_rows,
        preferred_element_type=jnp.float32,
    )
    return (new_max, running_sum, weighted)


def finish(state_now):
    _, running_sum, weighted = state_now
    result = weighted / running_sum[:, :, None]
    head_count, row_count = running_sum.shape
    return result.transpose(1, 0, 2).reshape(row_count, head_count * HEAD_DIM)


def gathered_body(
    ray_tokens,
    up_weight,
    down_weight,
    key_weight,
    value_weight,
    video_queries,
    video_keys,
    video_values,
    cross_queries,
):
    row_count = video_queries.shape[0]
    head_count = video_queries.shape[1] // HEAD_DIM
    up_full, down_full, key_full, value_full = (
        lax.all_gather(up_weight, "dp", axis=0, tiled=True),
        lax.all_gather(down_weight, "dp", axis=0, tiled=True),
        lax.all_gather(key_weight, "dp", axis=0, tiled=True),
        lax.all_gather(value_weight, "dp", axis=0, tiled=True),
    )
    normed = rms_normed(ray_tokens).astype(jnp.bfloat16)
    hidden = jax.nn.gelu(jnp.dot(normed, up_full, preferred_element_type=jnp.float32)).astype(
        jnp.bfloat16
    )
    partial_branch = lax.dot_general(
        hidden, down_full, (((1,), (1,)), ((), ())), preferred_element_type=jnp.float32
    )
    branch = lax.psum(partial_branch, "head")
    rays = (ray_tokens.astype(jnp.float32) + branch).astype(jnp.bfloat16)
    cross_heads = cross_queries.reshape(row_count, head_count, HEAD_DIM)
    piece = lax.all_gather(rays, ("view", "dp"), axis=0, tiled=True)
    piece_keys = jnp.dot(piece, key_full, preferred_element_type=jnp.float32).astype(jnp.bfloat16)
    piece_values = jnp.dot(piece, value_full, preferred_element_type=jnp.float32).astype(
        jnp.bfloat16
    )
    cross_state = absorb(empty_state(head_count, row_count), cross_heads, piece_keys, piece_values)
    cross = finish(cross_state)
    local_head_group = video_queries.reshape(row_count, head_count, HEAD_DIM)
    own_state = absorb(
        empty_state(head_count, row_count),
        local_head_group,
        lax.all_gather(video_keys, ("view", "dp"), axis=0, tiled=True),
        lax.all_gather(video_values, ("view", "dp"), axis=0, tiled=True),
    )
    own = finish(own_state)
    return (own + cross).astype(jnp.bfloat16)


VMEM = pl.BlockSpec(memory_space=pltpu.VMEM)
HBM = pl.BlockSpec(memory_space=pltpu.HBM)
SMEM = pl.BlockSpec(memory_space=pltpu.SMEM)
MIB = 2**20


def local_call(
    kernel, megabytes, flops, transcendentals, out_shape, scalars, *arrays, streamed=(), scratch=()
):
    moved = sum(array.size * array.dtype.itemsize for array in arrays + tuple(streamed))
    call = pl.pallas_call(
        kernel,
        in_specs=[SMEM] * len(scalars) + [VMEM] * len(arrays) + [HBM] * len(streamed),
        scratch_shapes=list(scratch),
        out_specs=jax.tree.map(lambda _: VMEM, out_shape),
        out_shape=out_shape,
        cost_estimate=pl.CostEstimate(
            flops=flops, transcendentals=transcendentals, bytes_accessed=moved
        ),
        compiler_params=pltpu.CompilerParams(vmem_limit_bytes=megabytes * MIB),
    )
    scalars = (scalar.astype(jnp.int32).reshape(1) for scalar in scalars)
    streamed = (pltpu.with_memory_space_constraint(array, pltpu.HBM) for array in streamed)
    return call(*scalars, *arrays, *streamed)


def matmul(left, right):
    return jnp.dot(left, right, preferred_element_type=jnp.float32)


def matmul_t(left, right):
    return lax.dot_general(
        left, right, (((1,), (1,)), ((), ())), preferred_element_type=jnp.float32
    )


def attend(query, keys, values):
    scores = matmul_t(query, keys)
    largest = jnp.max(scores, axis=1, keepdims=True)
    weights = jnp.exp2((scores - largest) * EXPONENT)
    total = jnp.sum(weights, axis=1, keepdims=True)
    return matmul(weights.astype(jnp.bfloat16), values) / total


def head_columns(head):
    if isinstance(head, int):
        return pl.ds(head * HEAD_DIM, HEAD_DIM)
    return pl.ds(pl.multiple_of(head * HEAD_DIM, HEAD_DIM), HEAD_DIM)


def pack_kernel(views, offset, view, side, *refs):
    sources, results, arrived = refs[: -views - 1], refs[-views - 1 : -1], refs[-1]
    span = sources[0].shape[1] // views
    copies = []
    for step, result in enumerate(results):
        start = pl.multiple_of((view[0] ^ step) * span + offset, HEAD_DIM)
        for slot, source in enumerate(sources[:3]):
            copies.append((source.at[:, pl.ds(start, result.shape[2])], result.at[slot]))
    for rays in sources[3:]:
        count, half = rays.shape[0], rays.shape[1] // 2
        for result in results:
            for block in range(half // HEAD_DIM):
                start = pl.multiple_of(side[0] * half + block * HEAD_DIM, HEAD_DIM)
                target = result.at[3, pl.ds(block * count, count)]
                copies.append((rays.at[:, pl.ds(start, HEAD_DIM)], target))
    copies = [
        pltpu.make_async_copy(source, target, arrived.at[index])
        for index, (source, target) in enumerate(copies)
    ]
    for copy in copies:
        copy.start()
    for copy in copies:
        copy.wait()


def pack(view, side, views, offset, width, *sources):
    rows, slots = sources[0].shape[0], len(sources)
    copies = 3 * views + (views * rows // sources[3].shape[0] if slots > 3 else 0)
    return local_call(
        functools.partial(pack_kernel, views, offset),
        8,
        sources[0].size,
        0,
        [jax.ShapeDtypeStruct((slots, rows, width), jnp.bfloat16)] * views,
        (view, side),
        streamed=sources,
        scratch=(pltpu.SemaphoreType.DMA((copies,)),),
    )


def unpack_kernel(count, *refs):
    pieces, result = refs[:-1], refs[-1]
    for index, piece in enumerate(pieces):
        rows = slice(index * count, (index + 1) * count)
        for block in range(result.shape[1] // HEAD_DIM):
            columns = slice(block * HEAD_DIM, (block + 1) * HEAD_DIM)
            result[rows, columns] = piece[3, block * count : (block + 1) * count]


def unpack(count, pieces):
    rows = pieces[0].shape[1]
    out_shape = jax.ShapeDtypeStruct((len(pieces) * count, rows * HEAD_DIM // count), jnp.bfloat16)
    kernel = functools.partial(unpack_kernel, count)
    return local_call(kernel, 4, rows * HEAD_DIM, 0, out_shape, (), *pieces)


def ray_kernel(aligned, here_ref, there_ref, *refs):
    sources, (keep, send), held, arrived = refs[:4], refs[4:6], refs[6:10], refs[10]
    copies = [
        pltpu.make_async_copy(source, target, arrived.at[index])
        for index, (source, target) in enumerate(zip(sources, held))
    ]
    for copy in copies:
        copy.start()
    same = aligned[0] == 1
    here, there = here_ref[...].astype(jnp.float32), there_ref[...].astype(jnp.float32)
    square = jnp.sum(here * here + there * there, axis=1, keepdims=True)
    factor = lax.rsqrt(square / (2 * here.shape[1]) + epsilon)
    here = (here * factor).astype(jnp.bfloat16)
    there = (there * factor).astype(jnp.bfloat16)
    near, far = jnp.where(same, here, there), jnp.where(same, there, here)
    copies[0].wait()
    copies[1].wait()
    hidden = jax.nn.gelu(matmul(near, held[0][...]) + matmul(far, held[1][...]))
    hidden = hidden.astype(jnp.bfloat16)
    copies[2].wait()
    branch_near = matmul_t(hidden, held[2][...])
    copies[3].wait()
    branch_far = matmul_t(hidden, held[3][...])
    keep[...] = jnp.where(same, branch_near, branch_far) + here_ref[...].astype(jnp.float32)
    send[...] = jnp.where(same, branch_far, branch_near)


def ray_layer(aligned, here, there, weights):
    return local_call(
        ray_kernel,
        20,
        8 * here.size * weights[0].shape[1],
        0,
        [jax.ShapeDtypeStruct(here.shape, jnp.float32)] * 2,
        (aligned,),
        here,
        there,
        streamed=weights,
        scratch=[pltpu.VMEM(weight.shape, weight.dtype) for weight in weights]
        + [pltpu.SemaphoreType.DMA((4,))],
    )


def own_kernel(views, *refs):
    arrays, results = refs[:-views], refs[-views:]
    offset = 0
    for start in range(0, len(arrays), 2 * views):
        pieces, others = arrays[start : start + views], arrays[start + views : start + 2 * views]

        @pl.loop(0, pieces[0].shape[2] // HEAD_DIM, unroll=True)
        def _(head, pieces=pieces, others=others, offset=offset):
            columns = head_columns(head)
            keys = jnp.concatenate([piece[0, :, columns] for piece in pieces + others], axis=0)
            values = jnp.concatenate([piece[1, :, columns] for piece in pieces + others], axis=0)
            for piece, result in zip(pieces, results):
                mixed = attend(piece[2, :, columns], keys, values)
                result[:, head_columns(head + offset)] = mixed.astype(jnp.bfloat16)

        offset += pieces[0].shape[2] // HEAD_DIM


def own_attention(sets):
    views = len(sets[0][0])
    rows = sets[0][0][0].shape[1]
    width = sum(pieces[0].shape[2] for pieces, _ in sets)
    area = 2 * views * views * rows * rows * (width // HEAD_DIM)
    out_shape = [jax.ShapeDtypeStruct((rows, width), jnp.bfloat16)] * views
    kernel = functools.partial(own_kernel, views)
    arrays = [array for pieces, others in sets for array in (*pieces, *others)]
    return local_call(kernel, 12, 4 * area * HEAD_DIM, area, out_shape, (), *arrays)


def cross_kernel(
    heads,
    aligned,
    here,
    there,
    peer_here,
    peer_there,
    key_near,
    key_far,
    value_near,
    value_far,
    query,
    result,
):
    same = aligned[0] == 1
    first = jnp.concatenate([here[...], peer_here[...]], axis=0)
    second = jnp.concatenate([there[...], peer_there[...]], axis=0)
    near, far = jnp.where(same, first, second), jnp.where(same, second, first)
    step = heads * HEAD_DIM

    @pl.loop(0, query.shape[1] // step)
    def _(group):
        block = pl.ds(pl.multiple_of(group * step, step), step)
        keys = (matmul(near, key_near[:, block]) + matmul(far, key_far[:, block])).astype(
            jnp.bfloat16
        )
        values = (matmul(near, value_near[:, block]) + matmul(far, value_far[:, block])).astype(
            jnp.bfloat16
        )
        for head in range(heads):
            inner = slice(head * HEAD_DIM, (head + 1) * HEAD_DIM)
            outer = head_columns(group * heads + head)
            result[:, outer] = attend(query[:, outer], keys[:, inner], values[:, inner])


def cross_attention(aligned, rays, weights, queries):
    rows, width = queries.shape
    ray_rows, depth = 2 * rays[0].shape[0], rays[0].shape[1]
    count = width // HEAD_DIM
    heads = max(group for group in range(1, 11) if count % group == 0)
    return local_call(
        functools.partial(cross_kernel, heads),
        20,
        8 * ray_rows * depth * width + 4 * rows * ray_rows * width,
        rows * ray_rows * count,
        jax.ShapeDtypeStruct((rows, width), jnp.float32),
        (aligned,),
        *rays,
        *weights,
        queries,
    )


def join_kernel(views, offsets, view, cross, *refs):
    pieces, result = refs[:-1], refs[-1]
    span = cross.shape[1] // views
    for index, piece in enumerate(pieces):
        chunk, step = divmod(index, views)
        start = pl.multiple_of((view[0] ^ step) * span + offsets[chunk], HEAD_DIM)
        columns = pl.ds(start, piece.shape[1])
        result[:, columns] = (cross[:, columns] + piece[...].astype(jnp.float32)).astype(
            jnp.bfloat16
        )


def join(view, cross, chunks, offsets):
    pieces = [piece for chunk in chunks for piece in chunk]
    kernel = functools.partial(join_kernel, len(chunks[0]), offsets)
    out_shape = jax.ShapeDtypeStruct(cross.shape, jnp.bfloat16)
    return local_call(kernel, 6, 2 * cross.size, 0, out_shape, (view,), cross, *pieces)


def swapped(values, axis):
    return lax.ppermute(values, axis, [(0, 1), (1, 0)])


def exchanged(values, views, step):
    return lax.ppermute(values, "view", [(i, i ^ step) for i in range(views)])


def exchanged_body(views, *arrays):
    return exchange_heads(views, *arrays)


def exchange_heads(
    views,
    ray_tokens,
    up_weight,
    down_weight,
    key_weight,
    value_weight,
    video_queries,
    video_keys,
    video_values,
    cross_queries,
):
    view, side, core = (lax.axis_index(axis) for axis in ("view", "head", "dp"))
    span = video_queries.shape[1] // views
    widths, groups = chunk_columns(span)
    offsets = [sum(widths[:index]) for index in range(len(widths))]
    aligned = side == core

    packed = [
        pack(
            view,
            side,
            views,
            *columns,
            video_keys,
            video_values,
            video_queries,
            *(() if index else (ray_tokens,)),
        )
        for index, columns in enumerate(zip(offsets, widths))
    ]
    up_peer = swapped(up_weight, "dp")
    down_peer = swapped(down_weight, "dp")
    key_peer = swapped(key_weight, "dp")
    value_peer = swapped(value_weight, "dp")

    chunks = [
        [exchanged(piece, views, step) if step else piece for step, piece in enumerate(pieces)]
        for pieces in packed
    ]

    ray_rows = unpack(ray_tokens.shape[0], chunks[0])
    other_half = swapped(ray_rows, "head")
    keep, send = ray_layer(
        aligned, ray_rows, other_half, (up_weight, up_peer, down_weight, down_peer)
    )
    here = (keep + swapped(send, "head")).astype(jnp.bfloat16)
    there = swapped(here, "head")
    rays = (here, there, swapped(here, "dp"), swapped(there, "dp"))
    cross = cross_attention(
        aligned, rays, (key_weight, key_peer, value_weight, value_peer), cross_queries
    )

    sets = [
        (
            pieces,
            [swapped(piece, "dp") for piece in pieces],
        )
        for pieces in chunks
    ]
    returned = []
    for members in groups:
        results = own_attention([sets[member] for member in members])
        returned.append(
            [exchanged(part, views, step) if step else part for step, part in enumerate(results)]
        )
    return join(view, cross, returned, [offsets[members[0]] for members in groups])


def chunk_columns(span):
    heads = span // HEAD_DIM
    early = (heads + 1) // 2
    counts = [1, early - 1, heads - early]
    groups = ((0, 1), (2,))
    return [count * HEAD_DIM for count in counts], groups


def solution(mesh):
    row_axes = ("groups", "view", "dp")
    in_specs = (P(row_axes, None),) + (P("dp", "head"),) * 4 + (P(row_axes, "head"),) * 4
    out_specs = P(row_axes, "head")

    views = mesh.shape["view"]

    def mapped(body):
        return jax.shard_map(
            body, mesh=mesh, in_specs=in_specs, out_specs=out_specs, check_vma=False
        )

    def whole(*arrays):
        span = arrays[5].shape[1] // mesh.shape["head"] // views
        exchange = (
            mesh.shape["dp"] == 2
            and mesh.shape["head"] == 2
            and views > 1
            and views & (views - 1) == 0
            and span % HEAD_DIM == 0
            and span >= 3 * HEAD_DIM
            and arrays[0].size * views == arrays[5].shape[0] * views * 2 * HEAD_DIM
        )
        if not exchange:
            return mapped(gathered_body)(*arrays)
        step = mapped(functools.partial(exchanged_body, views))
        return step(*arrays)

    return whole
```
